256 devices in a mesh: seq: 256 (over x, y, z, core).
Axes of the slice: x: 4, y: 4, z: 8, core: 2. Of those that a mesh axis runs over, the one named last changes fastest.
Arguments:
- tokens: bfloat16 [524288, 320], P('seq'), may hold values from -6 to 6
- w_in: bfloat16 [2, 320, 640], replicated, may hold values from -0.3125 to 0.3125
- b_in: float32 [2, 640], replicated, may hold values from -3 to 3
- w_out: bfloat16 [2, 640, 320], replicated, may hold values from -0.25 to 0.25
- b_out: float32 [2, 320], replicated, may hold values from -3 to 3
- cotangent: bfloat16 [524288, 320], P('seq'), may hold values from -6 to 6
Outputs:
- result: bfloat16 [524288, 320], P('seq')
- grad_tokens: bfloat16 [524288, 320], P('seq')
- grad_w_in: float32 [2, 320, 640], replicated
- grad_b_in: float32 [2, 640], replicated
- grad_w_out: float32 [2, 640, 320], replicated
- grad_b_out: float32 [2, 320], replicated
The draws below stay inside these ranges and needn't reach their ends.
All inputs are finite; a program needn't handle non-finite values.
Results may differ from the reference program's by a relative error of at most 0.0065.
Values may be sent and summed in bfloat16 or wider, within the bound.
No kernel may reach another device: no remote copies, remote signals or barrier semaphores. Data moves between devices by JAX's collectives and lax.ppermute only.
A program may use at most 128 MiB of HBM per device.

```python
import jax
import jax.numpy as jnp
from jax import lax

TRACKS = 20
TRACK_W = 16
D = 320
H = 640
LAYERS = 2
TOKENS = 524288


def shard_levels(key, extent, cuts, smallest, high):
    level, own = 1.0, jax.random.fold_in(key, 6)
    for position, shards_of in cuts:
        steps = jnp.exp(jax.random.uniform(jax.random.fold_in(own, position), (shards_of,), jnp.float32, smallest / len(cuts), high / len(cuts)))
        level = level * jnp.repeat(steps, extent[position] // shards_of).reshape([-1 if axis == position else 1 for axis in range(len(extent))])
    return level


def scatter_about(rng, extent, deviation, limit, cuts=(), kind=jnp.bfloat16):
    values = deviation * jax.random.normal(rng, extent, jnp.float32)
    if cuts:
        values = values * shard_levels(rng, extent, cuts, -0.22, 0.18)
    return jnp.clip(values, -limit, limit).astype(kind)


def setup_inputs(seed: int = 0) -> dict:
    streams_of = jax.random.split(jax.random.key(seed), 7)
    tokens = scatter_about(streams_of[0], (TOKENS, D), 1.0, 6.0, ((0, 256),))
    w_in = scatter_about(streams_of[1], (LAYERS, D, H), D ** -0.5, 0.3125)
    b_in = scatter_about(streams_of[2], (LAYERS, H), 0.5, 3.0, (), jnp.float32)
    w_out = scatter_about(streams_of[3], (LAYERS, H, D), H ** -0.5, 0.25)
    b_out = scatter_about(streams_of[4], (LAYERS, D), 0.5, 3.0, (), jnp.float32)
    cotangent = scatter_about(streams_of[5], (TOKENS, D), 1.0, 6.0, ((0, 256),))
    return {"tokens": tokens, "w_in": w_in, "b_in": b_in, "w_out": w_out, "b_out": b_out, "cotangent": cotangent}


def shift_of(track):
    if track == 0:
        return 0
    return min(2 ** (track - 1), TOKENS // 2)

def rotate(values, sign):
    pieces = []
    for track in range(TRACKS):
        block = values[:, track * TRACK_W:(track + 1) * TRACK_W]
        pieces.append(jnp.roll(block, sign * shift_of(track), axis=0))
    return jnp.concatenate(pieces, axis=1)

def gelu_tanh(t):
    return jax.nn.gelu(t, approximate=True)

def contract_rows(left, right):
    return lax.dot_general(left, right, (((0,), (0,)), ((), ())), preferred_element_type=jnp.float32)

def contract_cols(left, right):
    return lax.dot_general(left, right, (((1,), (1,)), ((), ())), preferred_element_type=jnp.float32)

def reference(tokens, w_in, b_in, w_out, b_out, cotangent):
    inputs = []
    current = tokens
    for layer in range(LAYERS):
        inputs.append(current)
        pre = jnp.dot(current, w_in[layer], preferred_element_type=jnp.float32) + b_in[layer]
        act = gelu_tanh(pre).astype(jnp.bfloat16)
        mixed = (current.astype(jnp.float32) + jnp.dot(act, w_out[layer], preferred_element_type=jnp.float32) + b_out[layer]).astype(jnp.bfloat16)
        current = rotate(mixed, 1)
    result = current
    scale = 1.0 / TOKENS ** 0.5
    grad = cotangent
    gw_in = [None] * LAYERS
    gb_in = [None] * LAYERS
    gw_out = [None] * LAYERS
    gb_out = [None] * LAYERS
    for layer in reversed(range(LAYERS)):
        back = rotate(grad, -1)
        layer_in = inputs[layer]
        pre = jnp.dot(layer_in, w_in[layer], preferred_element_type=jnp.float32) + b_in[layer]
        act = gelu_tanh(pre).astype(jnp.bfloat16)
        grad_act = contract_cols(back, w_out[layer])
        _, pull = jax.vjp(gelu_tanh, pre)
        delta = pull(grad_act)[0].astype(jnp.bfloat16)
        gw_out[layer] = contract_rows(act, back) * scale
        gb_out[layer] = lax.optimization_barrier(jnp.sum(back, axis=0, dtype=jnp.float32)) * scale
        gw_in[layer] = contract_rows(layer_in, delta) * scale
        gb_in[layer] = lax.optimization_barrier(jnp.sum(delta, axis=0, dtype=jnp.float32)) * scale
        grad = (back.astype(jnp.float32) + contract_cols(delta, w_in[layer])).astype(jnp.bfloat16)
    return (result, grad, jnp.stack(gw_in), jnp.stack(gb_in), jnp.stack(gw_out), jnp.stack(gb_out))
```

```python
import functools

import jax
import jax.numpy as jnp
from jax import lax
from jax.experimental import pallas as pl
from jax.experimental.pallas import tpu as pltpu
from jax.sharding import Mesh
from jax.sharding import PartitionSpec as P

TRACK_W = 16
TRACKS = 20
NEAR = 12
HOPS = (1, 2, 4, 8, 16, 32, 64, 128)
ALL = ("x", "y", "z", "c")
BLOCK = 512
LANES = 128
C0 = 0.7978845608028654
C1 = 0.044715
BF16 = jnp.bfloat16
F32 = jnp.float32

NT = (((1,), (1,)), ((), ()))
NN = (((1,), (0,)), ((), ()))


def dot(a, b, dims=NN):
    return lax.dot_general(a, b, dims, preferred_element_type=F32)


def margins(rows):
    out, at = [], rows
    for track in range(1, NEAR):
        size = max(LANES, 2 ** (track - 1))
        out.append((track, size, at))
        at += size
    return out, at


def put_pieces(v, at, near, first, far):
    top = NEAR * TRACK_W
    near[:, at] = v[:top]
    first[:, at] = v[top : top + TRACK_W]
    for i, ref in enumerate(far):
        lo = top + TRACK_W * (i + 1)
        ref[:, at] = v[lo : lo + TRACK_W]


def put_margins(near, first, sign):
    rows = near.shape[1]
    for track, size, at in margins(rows)[0]:
        lo = rows - size if sign > 0 else 0
        first[:, at : at + size] = near[track * TRACK_W : (track + 1) * TRACK_W, lo : lo + size]


def assemble(out, near, first, far, sign):
    rows = near.shape[1]
    out[0:TRACK_W, :] = near[0:TRACK_W, :]
    lane = lax.broadcasted_iota(jnp.int32, (TRACK_W, LANES), 1)
    for track, size, at in margins(rows)[0]:
        shift = 2 ** (track - 1)
        own = slice(track * TRACK_W, (track + 1) * TRACK_W)
        if shift < LANES:
            values = near[own, :].astype(F32)
            edge = first[:, at : at + LANES].astype(F32)
            if sign > 0:
                moved = pltpu.roll(values, shift, 1)
                edge = pltpu.roll(edge, shift, 1)
                head = jnp.where(lane < shift, edge, moved[:, :LANES])
                out[own, 0:LANES] = head.astype(BF16)
                out[own, LANES:rows] = moved[:, LANES:].astype(BF16)
            else:
                moved = pltpu.roll(values, rows - shift, 1)
                edge = pltpu.roll(edge, LANES - shift, 1)
                tail = jnp.where(lane >= LANES - shift, edge, moved[:, rows - LANES :])
                out[own, 0 : rows - LANES] = moved[:, : rows - LANES].astype(BF16)
                out[own, rows - LANES : rows] = tail.astype(BF16)
        elif sign > 0:
            out[own, 0:shift] = first[:, at : at + shift]
            out[own, shift:rows] = near[own, 0 : rows - shift]
        else:
            out[own, 0 : rows - shift] = near[own, shift:rows]
            out[own, rows - shift : rows] = first[:, at : at + shift]
    top = NEAR * TRACK_W
    out[top : top + TRACK_W, :] = first[:, 0:rows]
    for i, ref in enumerate(far):
        lo = top + TRACK_W * (i + 1)
        out[lo : lo + TRACK_W, :] = ref[...]


def over_blocks(rows, body):
    def step(i, carry):
        body(pl.ds(pl.multiple_of(i * BLOCK, BLOCK), BLOCK))
        return carry

    lax.fori_loop(0, rows // BLOCK, step, 0)


def flipped(x):
    return x.astype(F32).T


def split_kernel(cot, near, first, *far):
    over_blocks(cot.shape[0], lambda at: put_pieces(flipped(cot[at, :]).astype(BF16), at, near, first, far))
    put_margins(near, first, -1)


def gelu_parts(t):
    tanh = jnp.tanh(C0 * (t + C1 * (t * t * t)))
    half = 0.5 * (1.0 + tanh)
    slope = half + 0.5 * t * (1.0 - tanh * tanh) * (C0 + 3.0 * C0 * C1 * (t * t))
    return t * half, slope


def first_kernel(tokens, w_in_t, b_in, w_out_t, b_out, near, first, *far):
    def body(at):
        x = tokens[at, :]
        pre = dot(w_in_t[...], x, NT) + b_in[...]
        act = (0.5 * pre * (1.0 + jnp.tanh(C0 * (pre + C1 * (pre * pre * pre))))).astype(BF16)
        mixed = flipped(x) + dot(w_out_t[...], act) + b_out[...]
        put_pieces(mixed.astype(BF16), at, near, first, far)

    over_blocks(tokens.shape[0], body)
    put_margins(near, first, 1)


def backward(u, back, pre, w_out, w_in, acc_in, acc_out, acc_bi, acc_bo):
    act, slope = gelu_parts(pre)
    act = act.astype(BF16)
    delta = (dot(w_out[...], back) * slope).astype(BF16)
    grad = back.astype(F32) + dot(w_in[...], delta)
    ones = jnp.ones((TRACK_W, BLOCK), BF16)
    acc_in[...] += dot(u, delta, NT)
    acc_out[...] += dot(back, act, NT)
    acc_bi[...] += dot(ones, delta, NT)
    acc_bo[...] += dot(ones, back, NT)
    return act, grad


def put_sums(out, scale, acc_in, acc_out, acc_bi, acc_bo, bias):
    width, hidden = acc_in.shape
    for which, acc in enumerate((acc_in, acc_out)):
        for j in range(hidden // LANES):
            lo = (which * (hidden // LANES) + j) * width
            out[lo : lo + width, :] = (acc[:, j * LANES : (j + 1) * LANES] * scale).astype(BF16)
    lo = 2 * (hidden // LANES) * width
    out[lo:, :] = jnp.zeros((out.shape[0] - lo, LANES), BF16)
    bias[...] = jnp.zeros_like(bias)
    at = 0
    for acc in (acc_bi, acc_bo):
        n = acc.shape[1]
        for j in range(0, n, LANES):
            size = min(LANES, n - j)
            bias[at : at + 1, 0:size] = acc[0:1, j : j + size] * scale
            at += 1
    out[lo : lo + TRACK_W, :] = bias[...].astype(BF16)


def zero(*refs):
    for ref in refs:
        ref[...] = jnp.zeros_like(ref)


def middle_kernel(scale, n_far, *refs):
    n = n_far + 2
    un, uf, ufar = refs[0], refs[1], refs[2:n]
    bn, bf, bfar = refs[n], refs[n + 1], refs[n + 2 : 2 * n]
    w_in_t, b_in, w_out_t, b_out, w_in, w_out = refs[2 * n : 2 * n + 6]
    outs = refs[2 * n + 6 :]
    mn, mf, mfar = outs[0], outs[1], outs[2:n]
    gn, gf, gfar = outs[n], outs[n + 1], outs[n + 2 : 2 * n]
    sums = outs[2 * n]
    u_all, back_all, acc_in, acc_out, acc_bi, acc_bo, bias = outs[2 * n + 1 :]
    rows = un.shape[1]
    assemble(u_all, un, uf, ufar, 1)
    assemble(back_all, bn, bf, bfar, -1)
    zero(acc_in, acc_out, acc_bi, acc_bo)

    def body(at):
        u, back = u_all[:, at], back_all[:, at]
        pre = dot(w_in_t[...], u) + b_in[...]
        act, grad = backward(u, back, pre, w_out, w_in, acc_in, acc_out, acc_bi, acc_bo)
        put_pieces(grad.astype(BF16), at, gn, gf, gfar)
        mixed = u.astype(F32) + dot(w_out_t[...], act) + b_out[...]
        put_pieces(mixed.astype(BF16), at, mn, mf, mfar)

    over_blocks(rows, body)
    put_margins(gn, gf, -1)
    put_margins(mn, mf, 1)
    put_sums(sums, scale, acc_in, acc_out, acc_bi, acc_bo, bias)


def last_kernel(scale, n_far, *refs):
    n = n_far + 2
    bn, bf, bfar = refs[0], refs[1], refs[2:n]
    tokens, w_in_t, b_in, w_in, w_out = refs[n : n + 5]
    grad_tokens, sums, back_all, acc_in, acc_out, acc_bi, acc_bo, bias = refs[n + 5 :]
    assemble(back_all, bn, bf, bfar, -1)
    zero(acc_in, acc_out, acc_bi, acc_bo)

    def body(at):
        x, back = tokens[at, :], back_all[:, at]
        pre = dot(w_in_t[...], x, NT) + b_in[...]
        u = flipped(x).astype(BF16)
        _, grad = backward(u, back, pre, w_out, w_in, acc_in, acc_out, acc_bi, acc_bo)
        grad_tokens[at, :] = grad.T.astype(BF16)

    over_blocks(tokens.shape[0], body)
    put_sums(sums, scale, acc_in, acc_out, acc_bi, acc_bo, bias)


def join_kernel(n_far, near, first, *refs):
    far, (out, whole) = refs[:n_far], refs[n_far:]
    assemble(whole, near, first, far, 1)

    def body(at):
        out[at, :] = flipped(whole[:, at]).astype(BF16)

    over_blocks(near.shape[1], body)


def spread_kernel(width, hidden, core, mine, other, w_in, b_in, w_out, b_out, bias):
    blocks = hidden // LANES
    own = core[0]

    def layer_from(layer, ref):
        for j in range(blocks):
            w_in[layer, :, j * LANES : (j + 1) * LANES] = ref[j * width : (j + 1) * width, :].astype(F32)
            lo = (blocks + j) * width
            w_out[layer, j * LANES : (j + 1) * LANES, :] = ref[lo : lo + width, :].astype(F32).T
        lo = 2 * blocks * width
        bias[...] = ref[lo : lo + TRACK_W, :].astype(F32)
        at = 0
        for out, n in ((b_in, hidden), (b_out, width)):
            for j in range(0, n, LANES):
                size = min(LANES, n - j)
                out[layer : layer + 1, j : j + size] = bias[at : at + 1, 0:size]
                at += 1

    @pl.when(own == 0)
    def _():
        layer_from(0, mine)
        layer_from(1, other)

    @pl.when(own != 0)
    def _():
        layer_from(0, other)
        layer_from(1, mine)


def call(kernel, outs, args, scratch=(), flops=0, moved=0, smem=0):
    vmem = pl.BlockSpec(memory_space=pltpu.VMEM)
    return pl.pallas_call(
        kernel,
        out_shape=outs,
        in_specs=[pl.BlockSpec(memory_space=pltpu.SMEM)] * smem + [vmem] * (len(args) - smem),
        out_specs=jax.tree.map(lambda _: vmem, outs),
        scratch_shapes=list(scratch),
        cost_estimate=pl.CostEstimate(flops=flops, bytes_accessed=moved, transcendentals=0),
        compiler_params=pltpu.CompilerParams(vmem_limit_bytes=56 * 1024 * 1024),
    )(*args)


def passed(block, distance):
    n = lax.axis_size(ALL)
    return lax.ppermute(block, ALL, [((i - distance) % n, i) for i in range(n)])


def transfer(pieces, sign):
    near, first, *far = pieces
    far = [passed(v, sign * hop) for v, hop in zip(far[::-1], HOPS[:0:-1])][::-1]
    return (near, passed(first, sign), *far)


def local(tokens, w_in, b_in, w_out, b_out, cotangent):
    rows, width = tokens.shape
    layers, _, hidden = w_in.shape
    total = rows * lax.axis_size(ALL)
    scale = 1.0 / total**0.5
    n_far = len(HOPS) - 1
    pieces = [
        jax.ShapeDtypeStruct((NEAR * TRACK_W, rows), BF16),
        jax.ShapeDtypeStruct((TRACK_W, margins(rows)[1]), BF16),
    ] + [jax.ShapeDtypeStruct((TRACK_W, rows), BF16)] * n_far
    sums = jax.ShapeDtypeStruct((3328, LANES), BF16)
    whole = pltpu.VMEM((width, rows), BF16)
    accs = [
        pltpu.VMEM((width, hidden), F32),
        pltpu.VMEM((width, hidden), F32),
        pltpu.VMEM((TRACK_W, hidden), F32),
        pltpu.VMEM((TRACK_W, width), F32),
        pltpu.VMEM((TRACK_W, LANES), F32),
    ]
    product = 2 * rows * width * hidden
    block = 2 * rows * width
    w_in_t = jnp.swapaxes(w_in, 1, 2)
    w_out_t = jnp.swapaxes(w_out, 1, 2)
    b_in = b_in[:, :, None]
    b_out = b_out[:, :, None]

    back1 = transfer(call(split_kernel, pieces, (cotangent,), flops=product // 4, moved=2 * block), -1)
    u1 = transfer(
        call(
            first_kernel,
            pieces,
            (tokens, w_in_t[0], b_in[0], w_out_t[0], b_out[0]),
            flops=4 * product,
            moved=2 * block,
        ),
        1,
    )
    outs = call(
        functools.partial(middle_kernel, scale, n_far),
        pieces + pieces + [sums],
        (*u1, *back1, w_in_t[1], b_in[1], w_out_t[1], b_out[1], w_in[1], w_out[1]),
        [whole, whole] + accs,
        flops=12 * product,
        moved=4 * block,
    )
    n = n_far + 2
    back0 = transfer(outs[n : 2 * n], -1)
    shifted = transfer(outs[:n], 1)
    sums1 = outs[2 * n]
    devices = range(lax.axis_size(ALL))
    partner1 = lax.ppermute(sums1, ALL, [(i, i + 1) for i in devices if i % 2 == 0])
    grad_tokens, sums0 = call(
        functools.partial(last_kernel, scale, n_far),
        [jax.ShapeDtypeStruct((rows, width), BF16), sums],
        (*back0, tokens, w_in_t[0], b_in[0], w_in[0], w_out[0]),
        [whole] + accs,
        flops=10 * product,
        moved=3 * block,
    )
    partner0 = lax.ppermute(sums0, ALL, [(i + 1, i) for i in devices if i % 2 == 0])
    result = call(
        functools.partial(join_kernel, n_far),
        jax.ShapeDtypeStruct((rows, width), BF16),
        shifted,
        [whole],
        flops=product // 4,
        moved=2 * block,
    )
    core = lax.axis_index("c")
    kept = jnp.where(core == 0, sums0, sums1).astype(F32)
    kept = kept + jnp.where(core == 0, partner0, partner1).astype(F32)
    plane = lax.axis_size(("x", "y"))
    depth = lax.axis_size("z")
    part = kept.astype(BF16).reshape(plane, -1, LANES)
    part = lax.all_to_all(part, ("x", "y"), 0, 0, tiled=True)
    part = jnp.sum(part.astype(F32), axis=0).astype(BF16)
    part = part.reshape(depth, -1, LANES)
    part = lax.all_to_all(part, "z", 0, 0, tiled=True)
    part = jnp.sum(part.astype(F32), axis=0).astype(BF16)
    part = jnp.broadcast_to(part[None], (depth, *part.shape))
    part = lax.all_to_all(part, "z", 0, 0, tiled=True).reshape(1, -1, LANES)
    part = jnp.broadcast_to(part, (plane, *part.shape[1:]))
    mine = lax.all_to_all(part, ("x", "y"), 0, 0, tiled=True).reshape(-1, LANES)
    other = lax.ppermute(mine, ALL, [(i ^ 1, i) for i in devices])
    gw_in, gb_in, gw_out, gb_out = call(
        functools.partial(spread_kernel, width, hidden),
        [
            jax.ShapeDtypeStruct((layers, width, hidden), F32),
            jax.ShapeDtypeStruct((layers, hidden), F32),
            jax.ShapeDtypeStruct((layers, hidden, width), F32),
            jax.ShapeDtypeStruct((layers, width), F32),
        ],
        (core.astype(jnp.int32).reshape(1), mine, other),
        [pltpu.VMEM((TRACK_W, LANES), F32)],
        flops=product // 4,
        moved=4 * block,
        smem=1,
    )
    return result, grad_tokens, gw_in, gb_in, gw_out, gb_out


def solution(mesh):
    split = Mesh(mesh.devices.reshape(4, 4, 8, 2), ALL)
    rows = P(ALL, None)
    return jax.shard_map(
        local,
        mesh=split,
        in_specs=(rows, P(), P(), P(), P(), rows),
        out_specs=(rows, rows, P(), P(), P(), P()),
        check_vma=False,
    )
```

```python
import functools

import jax
import jax.numpy as jnp
from jax import lax
from jax.experimental import pallas as pl
from jax.experimental.pallas import tpu as pltpu
from jax.sharding import Mesh
from jax.sharding import PartitionSpec as P

TRACK_W = 16
TRACKS = 20
NEAR = 12
HOPS = (1, 2, 4, 8, 16, 32, 64, 128)
ALL = ("x", "y", "z", "c")
BLOCK = 512
LANES = 128
C0 = 0.7978845608028654
C1 = 0.044715
BF16 = jnp.bfloat16
F32 = jnp.float32

NT = (((1,), (1,)), ((), ()))
NN = (((1,), (0,)), ((), ()))


def dot(a, b, dims=NN):
    return lax.dot_general(a, b, dims, preferred_element_type=F32)


def margins(rows):
    out, at = [], rows
    for track in range(1, NEAR):
        size = max(LANES, 2 ** (track - 1))
        out.append((track, size, at))
        at += size
    return out, at


def put_pieces(v, at, near, first, far):
    near[:, at] = v[: NEAR * TRACK_W]
    put_far(v, at, first, far)


def put_far(v, at, first, far):
    top = NEAR * TRACK_W
    first[:, at] = v[top : top + TRACK_W]
    for i, ref in enumerate(far):
        lo = top + TRACK_W * (i + 1)
        ref[:, at] = v[lo : lo + TRACK_W]


def put_margins(near, first, sign):
    rows = near.shape[1]
    for track, size, at in margins(rows)[0]:
        lo = rows - size if sign > 0 else 0
        first[:, at : at + size] = near[track * TRACK_W : (track + 1) * TRACK_W, lo : lo + size]


def assemble(out, near, first, far, sign):
    rows = near.shape[1]
    out[0:TRACK_W, :] = near[0:TRACK_W, :]
    lane = lax.broadcasted_iota(jnp.int32, (TRACK_W, LANES), 1)
    for track, size, at in margins(rows)[0]:
        shift = 2 ** (track - 1)
        own = slice(track * TRACK_W, (track + 1) * TRACK_W)
        if shift < LANES:
            values = near[own, :].astype(F32)
            edge = first[:, at : at + LANES].astype(F32)
            if sign > 0:
                moved = pltpu.roll(values, shift, 1)
                edge = pltpu.roll(edge, shift, 1)
                head = jnp.where(lane < shift, edge, moved[:, :LANES])
                out[own, 0:LANES] = head.astype(BF16)
                out[own, LANES:rows] = moved[:, LANES:].astype(BF16)
            else:
                moved = pltpu.roll(values, rows - shift, 1)
                edge = pltpu.roll(edge, LANES - shift, 1)
                tail = jnp.where(lane >= LANES - shift, edge, moved[:, rows - LANES :])
                out[own, 0 : rows - LANES] = moved[:, : rows - LANES].astype(BF16)
                out[own, rows - LANES : rows] = tail.astype(BF16)
        elif sign > 0:
            out[own, 0:shift] = first[:, at : at + shift]
            out[own, shift:rows] = near[own, 0 : rows - shift]
        else:
            out[own, 0 : rows - shift] = near[own, shift:rows]
            out[own, rows - shift : rows] = first[:, at : at + shift]
    top = NEAR * TRACK_W
    out[top : top + TRACK_W, :] = first[:, 0:rows]
    for i, ref in enumerate(far):
        lo = top + TRACK_W * (i + 1)
        out[lo : lo + TRACK_W, :] = ref[...]


def over_blocks(rows, body):
    def step(i, carry):
        body(pl.ds(pl.multiple_of(i * BLOCK, BLOCK), BLOCK))
        return carry

    lax.fori_loop(0, rows // BLOCK, step, 0)


def column(row):
    wide = jnp.broadcast_to(row, (LANES, row.shape[1])).T
    return wide


def across(wide):
    return jnp.concatenate([wide] * (BLOCK // LANES), axis=1)


def turned(x):
    return x.astype(F32).T.astype(BF16)


def gelu_half(t):
    square = t * t
    return 0.5 + 0.5 * jnp.tanh(t * (C0 + (C0 * C1) * square)), square


def first_kernel(tokens, cot, w_in, b_in, w_out_t, b_out, *refs):
    near, first, far, cot_first, cot_far, shared, w_in_t = refs[0], refs[1], refs[2:8], refs[8], refs[9:15], refs[15], refs[16]
    wide_in, wide_out = refs[17:]
    up, down = shared.at[0:TRACK_W], shared.at[TRACK_W : 2 * TRACK_W]
    put_far(cot, slice(0, cot.shape[1]), cot_first, (*cot_far, down))
    put_margins(cot, cot_first, -1)
    w_in_t[...] = turned(w_in[0])
    wide_in[...] = column(b_in[0:1, :])
    wide_out[...] = column(b_out[0:1, :])

    def body(at):
        x = tokens[:, at]
        pre = dot(w_in_t[...], x) + across(wide_in[...])
        act = (pre * gelu_half(pre)[0]).astype(BF16)
        mixed = x.astype(F32) + dot(w_out_t[0], act) + across(wide_out[...])
        put_pieces(mixed.astype(BF16), at, near, first, (*far, up))

    over_blocks(tokens.shape[1], body)
    put_margins(near, first, 1)


def backward(u, back, pre, w_out, w_in, acc_in, acc_out, acc_bi, acc_bo):
    half, square = gelu_half(pre)
    act = pre * half
    slope = half + act * (1.0 - half) * (2.0 * C0 + (6.0 * C0 * C1) * square)
    act = act.astype(BF16)
    delta = (dot(w_out[...], back) * slope).astype(BF16)
    grad = back.astype(F32) + dot(w_in, delta)
    ones = jnp.ones((TRACK_W, BLOCK), BF16)
    acc_in[...] += dot(u, delta, NT)
    acc_out[...] += dot(back, act, NT)
    acc_bi[...] += dot(ones, delta, NT)
    acc_bo[...] += dot(ones, back, NT)
    return act, grad


def put_sums(out, scale, acc_in, acc_out, acc_bi, acc_bo, bias):
    width, hidden = acc_in.shape
    for which, acc in enumerate((acc_in, acc_out)):
        for j in range(hidden // LANES):
            lo = (which * (hidden // LANES) + j) * width
            out[lo : lo + width, :] = (acc[:, j * LANES : (j + 1) * LANES] * scale).astype(BF16)
    lo = 2 * (hidden // LANES) * width
    out[lo:, :] = jnp.zeros((out.shape[0] - lo, LANES), BF16)
    bias[...] = jnp.zeros_like(bias)
    at = 0
    for acc in (acc_bi, acc_bo):
        n = acc.shape[1]
        for j in range(0, n, LANES):
            size = min(LANES, n - j)
            bias[at : at + 1, 0:size] = acc[0:1, j : j + size] * scale
            at += 1
    out[lo : lo + TRACK_W, :] = bias[...].astype(BF16)


def zero(*refs):
    for ref in refs:
        ref[...] = jnp.zeros_like(ref)


def middle_kernel(scale, *refs):
    un, uf, ufar, cot, bf, bfar, shared = refs[0], refs[1], refs[2:8], refs[8], refs[9], refs[10:16], refs[16]
    w_in, b_in, w_out_t, b_out = refs[17:21]
    mn, mf, mfar, gn, gf, gfar, passing, sums = refs[21], refs[22], refs[23:29], refs[29], refs[30], refs[31:37], refs[37], refs[38]
    u_all, back_all, w_in_t, w_out, wide_in, wide_out, acc_in, acc_out, acc_bi, acc_bo, bias = refs[39:]
    w_in_t[...] = turned(w_in[1])
    w_out[...] = turned(w_out_t[1])
    wide_in[...] = column(b_in[1:2, :])
    wide_out[...] = column(b_out[1:2, :])
    assemble(u_all, un, uf, (*ufar, shared.at[0:TRACK_W]), 1)
    assemble(back_all, cot, bf, (*bfar, shared.at[TRACK_W : 2 * TRACK_W]), -1)
    zero(acc_in, acc_out, acc_bi, acc_bo)

    def body(at):
        u, back = u_all[:, at], back_all[:, at]
        pre = dot(w_in_t[...], u) + across(wide_in[...])
        act, grad = backward(u, back, pre, w_out, w_in[1], acc_in, acc_out, acc_bi, acc_bo)
        put_pieces(grad.astype(BF16), at, gn, gf, (*gfar, passing.at[TRACK_W : 2 * TRACK_W]))
        mixed = u.astype(F32) + dot(w_out_t[1], act) + across(wide_out[...])
        put_pieces(mixed.astype(BF16), at, mn, mf, (*mfar, passing.at[0:TRACK_W]))

    over_blocks(un.shape[1], body)
    put_margins(gn, gf, -1)
    put_margins(mn, mf, 1)
    put_sums(sums, scale, acc_in, acc_out, acc_bi, acc_bo, bias)


def last_kernel(scale, core, *refs):
    bn, bf, bfar, shared = refs[0], refs[1], refs[2:8], refs[8]
    tokens, w_in, w_in_t, b_in, w_out_t, sums1 = refs[9:15]
    grad_tokens, keep, send, back_all, w_out, wide_in, acc_in, acc_out, acc_bi, acc_bo, bias = refs[15:]
    w_out[...] = turned(w_out_t[0])
    wide_in[...] = column(b_in[0:1, :])
    assemble(back_all, bn, bf, (*bfar, shared.at[TRACK_W : 2 * TRACK_W]), -1)
    zero(acc_in, acc_out, acc_bi, acc_bo)

    def body(at):
        u, back = tokens[:, at], back_all[:, at]
        pre = dot(w_in_t[...], u) + across(wide_in[...])
        _, grad = backward(u, back, pre, w_out, w_in[0], acc_in, acc_out, acc_bi, acc_bo)
        grad_tokens[:, at] = grad.astype(BF16)

    over_blocks(tokens.shape[1], body)

    @pl.when(core[0] == 0)
    def _():
        put_sums(keep, scale, acc_in, acc_out, acc_bi, acc_bo, bias)
        send[...] = sums1[...]

    @pl.when(core[0] != 0)
    def _():
        put_sums(send, scale, acc_in, acc_out, acc_bi, acc_bo, bias)
        keep[...] = sums1[...]


def join_kernel(near, first, *refs):
    assemble(refs[7], near, first, (*refs[:6], refs[6].at[0:TRACK_W]), 1)


def sum_kernel(parts, out):
    total = parts[0].astype(F32)
    for i in range(1, parts.shape[0]):
        total += parts[i].astype(F32)
    for j in range(out.shape[0]):
        out[j] = total.astype(BF16)


def spread_kernel(width, hidden, core, mine, other, w_in, b_in, w_out_t, b_out, bias):
    blocks = hidden // LANES

    def layer_from(layer, ref):
        for j in range(blocks):
            columns = slice(j * LANES, (j + 1) * LANES)
            w_in[layer, :, columns] = ref[j * width : (j + 1) * width, :].astype(F32)
            lo = (blocks + j) * width
            w_out_t[layer, :, columns] = ref[lo : lo + width, :].astype(F32)
        lo = 2 * blocks * width
        bias[...] = ref[lo : lo + TRACK_W, :].astype(F32)
        at = 0
        for out, n in ((b_in, hidden), (b_out, width)):
            for j in range(0, n, LANES):
                size = min(LANES, n - j)
                out[layer : layer + 1, j : j + size] = bias[at : at + 1, 0:size]
                at += 1

    @pl.when(core[0] == 0)
    def _():
        layer_from(0, mine)
        layer_from(1, other)

    @pl.when(core[0] != 0)
    def _():
        layer_from(0, other)
        layer_from(1, mine)


def call(kernel, outs, args, scratch=(), flops=0, moved=0, smem=0, mib=24):
    vmem = pl.BlockSpec(memory_space=pltpu.VMEM)
    return pl.pallas_call(
        kernel,
        out_shape=outs,
        in_specs=[pl.BlockSpec(memory_space=pltpu.SMEM)] * smem + [vmem] * (len(args) - smem),
        out_specs=jax.tree.map(lambda _: vmem, outs),
        scratch_shapes=list(scratch),
        cost_estimate=pl.CostEstimate(flops=flops, bytes_accessed=moved, transcendentals=0),
        compiler_params=pltpu.CompilerParams(vmem_limit_bytes=mib * 1024 * 1024),
    )(*args)


def passed(block, distance):
    n = lax.axis_size(ALL)
    return lax.ppermute(block, ALL, [((i - distance) % n, i) for i in range(n)])


def transfer(first, far, sign):
    far = [passed(v, sign * hop) for v, hop in zip(far, HOPS[1:-1])]
    return (passed(first, sign), *far)


def local(tokens, w_in, b_in, w_out, b_out, cotangent):
    rows, width = tokens.shape
    layers, _, hidden = w_in.shape
    devices = range(lax.axis_size(ALL))
    scale = 1.0 / (rows * len(devices)) ** 0.5
    shape = jax.ShapeDtypeStruct
    near = shape((NEAR * TRACK_W, rows), BF16)
    first = shape((TRACK_W, margins(rows)[1]), BF16)
    far = [shape((TRACK_W, rows), BF16)] * (len(HOPS) - 2)
    shared = shape((2 * TRACK_W, rows), BF16)
    sums = shape((3328, LANES), BF16)
    whole = pltpu.VMEM((width, rows), BF16)
    weight = pltpu.VMEM((hidden, width), BF16)
    wide_in, wide_out = pltpu.VMEM((hidden, LANES), F32), pltpu.VMEM((width, LANES), F32)
    accs = [
        pltpu.VMEM((width, hidden), F32),
        pltpu.VMEM((width, hidden), F32),
        pltpu.VMEM((TRACK_W, hidden), F32),
        pltpu.VMEM((TRACK_W, width), F32),
        pltpu.VMEM((TRACK_W, LANES), F32),
    ]
    product = 2 * rows * width * hidden
    block = 2 * rows * width
    tokens, cotangent = tokens.T, cotangent.T
    w_out_t = jnp.swapaxes(w_out, 1, 2)
    core = lax.axis_index("c")
    core = core.astype(jnp.int32).reshape(1)

    outs = call(
        first_kernel,
        [near, first, *far, first, *far, shared, shape((hidden, width), BF16)],
        (tokens, cotangent, w_in, b_in, w_out_t, b_out),
        [wide_in, wide_out],
        flops=4 * product,
        moved=4 * block,
    )
    w_in_t0 = outs[16]
    shared0 = passed(outs[15], HOPS[-1])
    u1 = (outs[0], *transfer(outs[1], outs[2:8], 1))
    back1 = (cotangent, *transfer(outs[8], outs[9:15], -1))
    outs = call(
        functools.partial(middle_kernel, scale),
        [near, first, *far, near, first, *far, shared, sums],
        (*u1, *back1, shared0, w_in, b_in, w_out_t, b_out),
        [whole, whole, weight, weight, wide_in, wide_out] + accs,
        flops=12 * product,
        moved=4 * block,
    )
    shared1, sums1 = passed(outs[16], HOPS[-1]), outs[17]
    back0 = (outs[8], *transfer(outs[9], outs[10:16], -1))
    shifted = (outs[0], *transfer(outs[1], outs[2:8], 1))
    grad_tokens, keep, send = call(
        functools.partial(last_kernel, scale),
        [shape((width, rows), BF16), sums, sums],
        (core, *back0, shared1, tokens, w_in, w_in_t0, b_in, w_out_t, sums1),
        [whole, weight, wide_in] + accs,
        flops=10 * product,
        moved=3 * block,
        smem=1,
    )
    send, *shifted = lax.optimization_barrier((send, *shifted))
    partner = lax.ppermute(send, ALL, [(i ^ 1, i) for i in devices])
    result = call(join_kernel, shape((width, rows), BF16), (*shifted, shared1), flops=product // 4, moved=2 * block)
    plane = lax.axis_size(("x", "y"))
    depth = lax.axis_size("z")
    part = (keep.astype(F32) + partner.astype(F32)).astype(BF16).reshape(plane, -1, LANES)
    part = lax.all_to_all(part, ("x", "y"), 0, 0, tiled=True)
    part = call(sum_kernel, shape((depth, *part.shape[1:]), BF16), (part,), flops=block, moved=block, mib=8)
    part = lax.all_to_all(part, "z", 0, 0, tiled=True)
    part = call(sum_kernel, shape((plane, *part.shape[1:]), BF16), (part,), flops=block, moved=block, mib=8)
    mine = lax.all_to_all(part, ("x", "y"), 0, 0, tiled=True).reshape(-1, LANES)
    other = lax.ppermute(mine, ALL, [(i ^ 1, i) for i in devices])
    gw_in, gb_in, gw_out_t, gb_out = call(
        functools.partial(spread_kernel, width, hidden),
        [
            shape((layers, width, hidden), F32),
            shape((layers, hidden), F32),
            shape((layers, width, hidden), F32),
            shape((layers, width), F32),
        ],
        (core, mine, other),
        [pltpu.VMEM((TRACK_W, LANES), F32)],
        flops=product // 4,
        moved=4 * block,
        smem=1,
    )
    return result.T, grad_tokens.T, gw_in, gb_in, jnp.swapaxes(gw_out_t, 1, 2), gb_out


def solution(mesh):
    split = Mesh(mesh.devices.reshape(4, 4, 8, 2), ALL)
    rows = P(ALL, None)
    return jax.shard_map(
        local,
        mesh=split,
        in_specs=(rows, P(), P(), P(), P(), rows),
        out_specs=(rows, rows, P(), P(), P(), P()),
        check_vma=False,
    )
```

```python
import functools

import jax
import jax.numpy as jnp
from jax import lax
from jax.experimental import pallas as pl
from jax.experimental.pallas import tpu as pltpu
from jax.sharding import Mesh
from jax.sharding import PartitionSpec as P

TRACK_W = 16
TRACKS = 20
NEAR = 12
HOPS = (1, 2, 4, 8, 16, 32, 64, 128)
ALL = ("x", "y", "z", "c")
BLOCK = 512
LANES = 128
C0 = 0.7978845608028654
C1 = 0.044715
BF16 = jnp.bfloat16
F32 = jnp.float32

NT = (((1,), (1,)), ((), ()))
NN = (((1,), (0,)), ((), ()))


def dot(a, b, dims=NN):
    return lax.dot_general(a, b, dims, preferred_element_type=F32)


def margins(rows):
    out, at = [], rows
    for track in range(1, NEAR):
        size = max(LANES, 2 ** (track - 1))
        out.append((track, size, at))
        at += size
    return out, at


def put_pieces(v, at, near, first, far):
    near[:, at] = v[: NEAR * TRACK_W]
    put_far(v, at, first, far)


def put_far(v, at, first, far):
    top = NEAR * TRACK_W
    first[:, at] = v[top : top + TRACK_W]
    for i, ref in enumerate(far):
        lo = top + TRACK_W * (i + 1)
        ref[:, at] = v[lo : lo + TRACK_W]


def put_margins(near, first, sign):
    rows = near.shape[1]
    for track, size, at in margins(rows)[0]:
        lo = rows - size if sign > 0 else 0
        first[:, at : at + size] = near[track * TRACK_W : (track + 1) * TRACK_W, lo : lo + size]


def assemble(out, near, first, far, sign):
    rows = near.shape[1]
    out[0:TRACK_W, :] = near[0:TRACK_W, :]
    lane = lax.broadcasted_iota(jnp.int32, (TRACK_W, LANES), 1)
    for track, size, at in margins(rows)[0]:
        shift = 2 ** (track - 1)
        own = slice(track * TRACK_W, (track + 1) * TRACK_W)
        if shift < LANES:
            values = near[own, :].astype(F32)
            edge = first[:, at : at + LANES].astype(F32)
            if sign > 0:
                moved = pltpu.roll(values, shift, 1)
                edge = pltpu.roll(edge, shift, 1)
                head = jnp.where(lane < shift, edge, moved[:, :LANES])
                out[own, 0:LANES] = head.astype(BF16)
                out[own, LANES:rows] = moved[:, LANES:].astype(BF16)
            else:
                moved = pltpu.roll(values, rows - shift, 1)
                edge = pltpu.roll(edge, LANES - shift, 1)
                tail = jnp.where(lane >= LANES - shift, edge, moved[:, rows - LANES :])
                out[own, 0 : rows - LANES] = moved[:, : rows - LANES].astype(BF16)
                out[own, rows - LANES : rows] = tail.astype(BF16)
        elif sign > 0:
            out[own, 0:shift] = first[:, at : at + shift]
            out[own, shift:rows] = near[own, 0 : rows - shift]
        else:
            out[own, 0 : rows - shift] = near[own, shift:rows]
            out[own, rows - shift : rows] = first[:, at : at + shift]
    top = NEAR * TRACK_W
    out[top : top + TRACK_W, :] = first[:, 0:rows]
    for i, ref in enumerate(far):
        lo = top + TRACK_W * (i + 1)
        out[lo : lo + TRACK_W, :] = ref[...]


def over_blocks(rows, body):
    def step(i, carry):
        body(pl.ds(pl.multiple_of(i * BLOCK, BLOCK), BLOCK))
        return carry

    lax.fori_loop(0, rows // BLOCK, step, 0)


def column(row):
    wide = jnp.broadcast_to(row, (LANES, row.shape[1])).T
    return wide


def across(wide):
    return jnp.concatenate([wide] * (BLOCK // LANES), axis=1)


def turned(x):
    return x.astype(F32).T.astype(BF16)


def gelu_half(t):
    square = t * t
    return 0.5 + 0.5 * jnp.tanh(t * (C0 + (C0 * C1) * square)), square


def brought(sems, pairs):
    copies = [pltpu.make_async_copy(source, target, sems.at[i]) for i, (source, target) in enumerate(pairs)]
    for copy in copies:
        copy.start()
    return copies


def first_kernel(tokens, cot, w_in, b_in, w_out_t, b_out, *refs):
    near, first, far, cot_first, cot_far, shared = refs[0], refs[1], refs[2:8], refs[8], refs[9:15], refs[15]
    x_all, w_here, w_in_t, w_out_here, b_in_here, b_out_here, wide_in, wide_out, sems = refs[16:]
    rows = tokens.shape[1]
    up, down = shared.at[0:TRACK_W], shared.at[TRACK_W : 2 * TRACK_W]
    top = NEAR * TRACK_W
    pairs = [
        (w_in.at[0], w_here),
        (b_in, b_in_here),
        (tokens, x_all),
        (w_out_t.at[0], w_out_here),
        (b_out, b_out_here),
        (cot.at[top : top + TRACK_W], cot_first.at[:, 0:rows]),
    ]
    for i, ref in enumerate((*cot_far, down)):
        lo = top + TRACK_W * (i + 1)
        pairs.append((cot.at[lo : lo + TRACK_W], ref))
    for track, size, at in margins(rows)[0]:
        own = slice(track * TRACK_W, (track + 1) * TRACK_W)
        pairs.append((cot.at[own, 0:size], cot_first.at[:, at : at + size]))
    copies = brought(sems, pairs)
    copies[0].wait()
    w_in_t[...] = turned(w_here[...])
    copies[1].wait()
    wide_in[...] = column(b_in_here[0:1, :])
    for copy in copies[2:5]:
        copy.wait()
    wide_out[...] = column(b_out_here[0:1, :])

    def body(at):
        x = x_all[:, at]
        pre = dot(w_in_t[...], x) + across(wide_in[...])
        act = (pre * gelu_half(pre)[0]).astype(BF16)
        mixed = x.astype(F32) + dot(w_out_here[...], act) + across(wide_out[...])
        put_pieces(mixed.astype(BF16), at, near, first, (*far, up))

    over_blocks(rows, body)
    put_margins(near, first, 1)
    for copy in copies[5:]:
        copy.wait()


def backward(u, back, pre, w_out, w_in, acc_in, acc_out, acc_bi, acc_bo):
    half, square = gelu_half(pre)
    act = pre * half
    slope = half + act * (1.0 - half) * (2.0 * C0 + (6.0 * C0 * C1) * square)
    act = act.astype(BF16)
    delta = (dot(w_out[...], back) * slope).astype(BF16)
    grad = back.astype(F32) + dot(w_in, delta)
    ones = jnp.ones((TRACK_W, BLOCK), BF16)
    acc_in[...] += dot(u, delta, NT)
    acc_out[...] += dot(back, act, NT)
    acc_bi[...] += dot(ones, delta, NT)
    acc_bo[...] += dot(ones, back, NT)
    return act, grad


def put_sums(out, scale, acc_in, acc_out, acc_bi, acc_bo, bias):
    width, hidden = acc_in.shape
    for which, acc in enumerate((acc_in, acc_out)):
        for j in range(hidden // LANES):
            lo = (which * (hidden // LANES) + j) * width
            out[lo : lo + width, :] = (acc[:, j * LANES : (j + 1) * LANES] * scale).astype(BF16)
    lo = 2 * (hidden // LANES) * width
    out[lo:, :] = jnp.zeros((out.shape[0] - lo, LANES), BF16)
    bias[...] = jnp.zeros_like(bias)
    at = 0
    for acc in (acc_bi, acc_bo):
        n = acc.shape[1]
        for j in range(0, n, LANES):
            size = min(LANES, n - j)
            bias[at : at + 1, 0:size] = acc[0:1, j : j + size] * scale
            at += 1
    out[lo : lo + TRACK_W, :] = bias[...].astype(BF16)


def zero(*refs):
    for ref in refs:
        ref[...] = jnp.zeros_like(ref)


def middle_kernel(scale, *refs):
    un, uf, ufar, cot, bf, bfar, shared = refs[0], refs[1], refs[2:8], refs[8], refs[9], refs[10:16], refs[16]
    w_in, b_in, w_out_t, b_out = refs[17:21]
    mn, mf, mfar, gn, gf, gfar, passing, sums = refs[21], refs[22], refs[23:29], refs[29], refs[30], refs[31:37], refs[37], refs[38]
    u_all, back_all, w_in_t, w_out, wide_in, wide_out, acc_in, acc_out, acc_bi, acc_bo, bias = refs[39:]
    w_in_t[...] = turned(w_in[1])
    w_out[...] = turned(w_out_t[1])
    wide_in[...] = column(b_in[1:2, :])
    wide_out[...] = column(b_out[1:2, :])
    assemble(u_all, un, uf, (*ufar, shared.at[0:TRACK_W]), 1)
    assemble(back_all, cot, bf, (*bfar, shared.at[TRACK_W : 2 * TRACK_W]), -1)
    zero(acc_in, acc_out, acc_bi, acc_bo)

    def body(at):
        u, back = u_all[:, at], back_all[:, at]
        pre = dot(w_in_t[...], u) + across(wide_in[...])
        act, grad = backward(u, back, pre, w_out, w_in[1], acc_in, acc_out, acc_bi, acc_bo)
        put_pieces(grad.astype(BF16), at, gn, gf, (*gfar, passing.at[TRACK_W : 2 * TRACK_W]))
        mixed = u.astype(F32) + dot(w_out_t[1], act) + across(wide_out[...])
        put_pieces(mixed.astype(BF16), at, mn, mf, (*mfar, passing.at[0:TRACK_W]))

    over_blocks(un.shape[1], body)
    put_margins(gn, gf, -1)
    put_margins(mn, mf, 1)
    put_sums(sums, scale, acc_in, acc_out, acc_bi, acc_bo, bias)


def last_kernel(scale, tokens, w_in, b_in, w_out_t, sums1, *refs):
    bn, bf, bfar, shared = refs[0], refs[1], refs[2:8], refs[8]
    grad_tokens, keep, send, w_in_t, w_out, back_all, wide_in, acc_in, acc_out, acc_bi, acc_bo, bias = refs[9:]
    core = lax.axis_index("c")
    zero(acc_in, acc_out, acc_bi, acc_bo)
    w_in_t[...] = turned(w_in[0])
    w_out[...] = turned(w_out_t[0])
    wide_in[...] = column(b_in[0:1, :])
    assemble(back_all, bn, bf, (*bfar, shared.at[TRACK_W : 2 * TRACK_W]), -1)

    def body(at):
        u, back = tokens[:, at], back_all[:, at]
        pre = dot(w_in_t[...], u) + across(wide_in[...])
        _, grad = backward(u, back, pre, w_out, w_in[0], acc_in, acc_out, acc_bi, acc_bo)
        grad_tokens[:, at] = grad.astype(BF16)

    over_blocks(tokens.shape[1], body)

    @pl.when(core == 0)
    def _():
        put_sums(keep, scale, acc_in, acc_out, acc_bi, acc_bo, bias)
        send[...] = sums1[...]

    @pl.when(core != 0)
    def _():
        put_sums(send, scale, acc_in, acc_out, acc_bi, acc_bo, bias)
        keep[...] = sums1[...]


def join_kernel(near, first, *refs):
    assemble(refs[7], near, first, (*refs[:6], refs[6].at[0:TRACK_W]), 1)


def sum_kernel(parts, out):
    total = parts[0].astype(F32)
    for i in range(1, parts.shape[0]):
        total += parts[i].astype(F32)
    for j in range(out.shape[0]):
        out[j] = total.astype(BF16)


def spread_kernel(width, hidden, mine, other, w_in, b_in, w_out_t, b_out, bias):
    blocks = hidden // LANES

    def layer_from(layer, ref):
        for j in range(blocks):
            columns = slice(j * LANES, (j + 1) * LANES)
            w_in[layer, :, columns] = ref[j * width : (j + 1) * width, :].astype(F32)
            lo = (blocks + j) * width
            w_out_t[layer, :, columns] = ref[lo : lo + width, :].astype(F32)
        lo = 2 * blocks * width
        bias[...] = ref[lo : lo + TRACK_W, :].astype(F32)
        at = 0
        for out, n in ((b_in, hidden), (b_out, width)):
            for j in range(0, n, LANES):
                size = min(LANES, n - j)
                out[layer : layer + 1, j : j + size] = bias[at : at + 1, 0:size]
                at += 1

    @pl.when(lax.axis_index("c") == 0)
    def _():
        layer_from(0, mine)
        layer_from(1, other)

    @pl.when(lax.axis_index("c") != 0)
    def _():
        layer_from(0, other)
        layer_from(1, mine)


def call(kernel, outs, args, scratch=(), flops=0, moved=0, hbm=0, mib=24):
    vmem = pl.BlockSpec(memory_space=pltpu.VMEM)
    return pl.pallas_call(
        kernel,
        out_shape=outs,
        in_specs=[pl.BlockSpec(memory_space=pltpu.HBM)] * hbm + [vmem] * (len(args) - hbm),
        out_specs=jax.tree.map(lambda _: vmem, outs),
        scratch_shapes=list(scratch),
        cost_estimate=pl.CostEstimate(flops=flops, bytes_accessed=moved, transcendentals=0),
        compiler_params=pltpu.CompilerParams(vmem_limit_bytes=mib * 1024 * 1024),
    )(*args)


def passed(block, distance):
    n = lax.axis_size(ALL)
    return lax.ppermute(block, ALL, [((i - distance) % n, i) for i in range(n)])


def transfer(first, far, sign):
    far = [passed(v, sign * hop) for v, hop in zip(far, HOPS[1:-1])]
    return (passed(first, sign), *far)


def local(tokens, w_in, b_in, w_out, b_out, cotangent):
    rows, width = tokens.shape
    layers, _, hidden = w_in.shape
    devices = range(lax.axis_size(ALL))
    scale = 1.0 / (rows * len(devices)) ** 0.5
    shape = jax.ShapeDtypeStruct
    near = shape((NEAR * TRACK_W, rows), BF16)
    first = shape((TRACK_W, margins(rows)[1]), BF16)
    far = [shape((TRACK_W, rows), BF16)] * (len(HOPS) - 2)
    shared = shape((2 * TRACK_W, rows), BF16)
    sums = shape((3328, LANES), BF16)
    whole = pltpu.VMEM((width, rows), BF16)
    weight = pltpu.VMEM((hidden, width), BF16)
    wide_in, wide_out = pltpu.VMEM((hidden, LANES), F32), pltpu.VMEM((width, LANES), F32)
    accs = [
        pltpu.VMEM((width, hidden), F32),
        pltpu.VMEM((width, hidden), F32),
        pltpu.VMEM((TRACK_W, hidden), F32),
        pltpu.VMEM((TRACK_W, width), F32),
        pltpu.VMEM((TRACK_W, LANES), F32),
    ]
    product = 2 * rows * width * hidden
    block = 2 * rows * width
    tokens, cotangent = tokens.T, cotangent.T
    w_out_t = jnp.swapaxes(w_out, 1, 2)
    outs = call(
        first_kernel,
        [near, first, *far, first, *far, shared],
        (tokens, cotangent, w_in, b_in, w_out_t, b_out),
        [
            whole,
            pltpu.VMEM((width, hidden), BF16),
            weight,
            pltpu.VMEM((width, hidden), BF16),
            pltpu.VMEM((layers, hidden), F32),
            pltpu.VMEM((layers, width), F32),
            wide_in,
            wide_out,
            pltpu.SemaphoreType.DMA((6 + len(HOPS) - 1 + NEAR - 1,)),
        ],
        flops=4 * product,
        moved=4 * block,
        hbm=6,
        mib=62,
    )
    shared0 = passed(outs[15], HOPS[-1])
    u1 = (outs[0], *transfer(outs[1], outs[2:8], 1))
    back1 = (cotangent, *transfer(outs[8], outs[9:15], -1))
    outs = call(
        functools.partial(middle_kernel, scale),
        [near, first, *far, near, first, *far, shared, sums],
        (*u1, *back1, shared0, w_in, b_in, w_out_t, b_out),
        [whole, whole, weight, weight, wide_in, wide_out] + accs,
        flops=12 * product,
        moved=4 * block,
    )
    shared1, sums1 = passed(outs[16], HOPS[-1]), outs[17]
    back0 = (outs[8], *transfer(outs[9], outs[10:16], -1))
    shifted = (outs[0], *transfer(outs[1], outs[2:8], 1))
    grad_tokens, keep, send = call(
        functools.partial(last_kernel, scale),
        [shape((width, rows), BF16), sums, sums],
        (tokens, w_in, b_in, w_out_t, sums1, *back0, shared1),
        [weight, weight, whole, wide_in, *accs],
        flops=10 * product,
        moved=3 * block,
    )
    send, *shifted = lax.optimization_barrier((send, *shifted))
    partner = lax.ppermute(send, ALL, [(i ^ 1, i) for i in devices])
    result = call(join_kernel, shape((width, rows), BF16), (*shifted, shared1), flops=product // 4, moved=2 * block)
    plane = lax.axis_size(("x", "y"))
    depth = lax.axis_size("z")
    part = (keep.astype(F32) + partner.astype(F32)).astype(BF16).reshape(plane, -1, LANES)
    part = lax.all_to_all(part, ("x", "y"), 0, 0, tiled=True)
    part = call(sum_kernel, shape((depth, *part.shape[1:]), BF16), (part,), flops=block, moved=block, mib=8)
    part = lax.all_to_all(part, "z", 0, 0, tiled=True)
    part = call(sum_kernel, shape((plane, *part.shape[1:]), BF16), (part,), flops=block, moved=block, mib=8)
    mine = lax.all_to_all(part, ("x", "y"), 0, 0, tiled=True).reshape(-1, LANES)
    other = lax.ppermute(mine, ALL, [(i ^ 1, i) for i in devices])
    gw_in, gb_in, gw_out_t, gb_out = call(
        functools.partial(spread_kernel, width, hidden),
        [
            shape((layers, width, hidden), F32),
            shape((layers, hidden), F32),
            shape((layers, width, hidden), F32),
            shape((layers, width), F32),
        ],
        (mine, other),
        [pltpu.VMEM((TRACK_W, LANES), F32)],
        flops=product // 4,
        moved=4 * block,
    )
    return result.T, grad_tokens.T, gw_in, gb_in, jnp.swapaxes(gw_out_t, 1, 2), gb_out


def solution(mesh):
    split = Mesh(mesh.devices.reshape(4, 4, 8, 2), ALL)
    rows = P(ALL, None)
    return jax.shard_map(
        local,
        mesh=split,
        in_specs=(rows, P(), P(), P(), P(), rows),
        out_specs=(rows, rows, P(), P(), P(), P()),
        check_vma=False,
    )
```

```python
import functools

import jax
import jax.numpy as jnp
from jax import lax
from jax.experimental import pallas as pl
from jax.experimental.pallas import tpu as pltpu
from jax.sharding import Mesh
from jax.sharding import PartitionSpec as P

TRACK_W = 16
TRACKS = 20
NEAR = 12
HOPS = (1, 2, 4, 8, 16, 32, 64, 128)
ORDER = (2, 1, 0, 4, 3, 5)
ALL = ("x", "y", "z", "c")
BLOCK = 512
LANES = 128
C0 = 0.7978845608028654
C1 = 0.044715
BF16 = jnp.bfloat16
F32 = jnp.float32

NT = (((1,), (1,)), ((), ()))
NN = (((1,), (0,)), ((), ()))


def dot(a, b, dims=NN):
    return lax.dot_general(a, b, dims, preferred_element_type=F32)


def margins(rows):
    out, at = [], rows
    for track in range(1, NEAR):
        size = max(LANES, 2 ** (track - 1))
        out.append((track, size, at))
        at += size
    return out, at


def put_pieces(v, at, near, first, far):
    near[:, at] = v[: NEAR * TRACK_W]
    put_far(v, at, first, far)


def put_far(v, at, first, far):
    top = NEAR * TRACK_W
    first[:, at] = v[top : top + TRACK_W]
    for i, ref in enumerate(far):
        lo = top + TRACK_W * (i + 1)
        ref[:, at] = v[lo : lo + TRACK_W]


def put_margins(near, first, sign):
    rows = near.shape[1]
    for track, size, at in margins(rows)[0]:
        lo = rows - size if sign > 0 else 0
        first[:, at : at + size] = near[track * TRACK_W : (track + 1) * TRACK_W, lo : lo + size]


def assemble(out, near, first, far, sign):
    rows = near.shape[1]
    out[0:TRACK_W, :] = near[0:TRACK_W, :]
    lane = lax.broadcasted_iota(jnp.int32, (TRACK_W, LANES), 1)
    for track, size, at in margins(rows)[0]:
        shift = 2 ** (track - 1)
        own = slice(track * TRACK_W, (track + 1) * TRACK_W)
        if shift < LANES:
            values = near[own, :].astype(F32)
            edge = first[:, at : at + LANES].astype(F32)
            if sign > 0:
                moved = pltpu.roll(values, shift, 1)
                edge = pltpu.roll(edge, shift, 1)
                head = jnp.where(lane < shift, edge, moved[:, :LANES])
                out[own, 0:LANES] = head.astype(BF16)
                out[own, LANES:rows] = moved[:, LANES:].astype(BF16)
            else:
                moved = pltpu.roll(values, rows - shift, 1)
                edge = pltpu.roll(edge, LANES - shift, 1)
                tail = jnp.where(lane >= LANES - shift, edge, moved[:, rows - LANES :])
                out[own, 0 : rows - LANES] = moved[:, : rows - LANES].astype(BF16)
                out[own, rows - LANES : rows] = tail.astype(BF16)
        elif sign > 0:
            out[own, 0:shift] = first[:, at : at + shift]
            out[own, shift:rows] = near[own, 0 : rows - shift]
        else:
            out[own, 0 : rows - shift] = near[own, shift:rows]
            out[own, rows - shift : rows] = first[:, at : at + shift]
    top = NEAR * TRACK_W
    out[top : top + TRACK_W, :] = first[:, 0:rows]
    for i, ref in enumerate(far):
        lo = top + TRACK_W * (i + 1)
        out[lo : lo + TRACK_W, :] = ref[...]


def over_blocks(rows, body):
    def step(i, carry):
        body(pl.ds(pl.multiple_of(i * BLOCK, BLOCK), BLOCK))
        return carry

    lax.fori_loop(0, rows // BLOCK, step, 0)


def column(row):
    wide = jnp.broadcast_to(row, (LANES, row.shape[1])).T
    return wide


def across(wide):
    return jnp.concatenate([wide] * (BLOCK // LANES), axis=1)


def turned(x):
    return x.astype(F32).T.astype(BF16)


def gelu_half(t):
    square = t * t
    return 0.5 + 0.5 * jnp.tanh(t * (C0 + (C0 * C1) * square)), square


def brought(sems, pairs):
    copies = [pltpu.make_async_copy(source, target, sems.at[i]) for i, (source, target) in enumerate(pairs)]
    for copy in copies:
        copy.start()
    return copies


def first_kernel(tokens, cot, w_in, b_in, w_out_t, b_out, *refs):
    near, first, far, cot_first, cot_far, shared = refs[0], refs[1], refs[2:8], refs[8], refs[9:15], refs[15]
    x_all, w_here, w_in_t, w_out_here, b_in_here, b_out_here, wide_in, wide_out, sems = refs[16:]
    rows = tokens.shape[1]
    up, down = shared.at[0:TRACK_W], shared.at[TRACK_W : 2 * TRACK_W]
    top = NEAR * TRACK_W
    pairs = [
        (w_in.at[0], w_here),
        (b_in, b_in_here),
        (tokens, x_all),
        (w_out_t.at[0], w_out_here),
        (b_out, b_out_here),
        (cot.at[top : top + TRACK_W], cot_first.at[:, 0:rows]),
    ]
    for i, ref in enumerate((*cot_far, down)):
        lo = top + TRACK_W * (i + 1)
        pairs.append((cot.at[lo : lo + TRACK_W], ref))
    for track, size, at in margins(rows)[0]:
        own = slice(track * TRACK_W, (track + 1) * TRACK_W)
        pairs.append((cot.at[own, 0:size], cot_first.at[:, at : at + size]))
    copies = brought(sems, pairs)
    copies[0].wait()
    w_in_t[...] = turned(w_here[...])
    copies[1].wait()
    wide_in[...] = column(b_in_here[0:1, :])
    for copy in copies[2:5]:
        copy.wait()
    wide_out[...] = column(b_out_here[0:1, :])

    def body(at):
        x = x_all[:, at]
        pre = dot(w_in_t[...], x) + across(wide_in[...])
        act = (pre * gelu_half(pre)[0]).astype(BF16)
        mixed = x.astype(F32) + dot(w_out_here[...], act) + across(wide_out[...])
        put_pieces(mixed.astype(BF16), at, near, first, (*far, up))

    over_blocks(rows, body)
    put_margins(near, first, 1)
    for copy in copies[5:]:
        copy.wait()


def backward(u, back, pre, w_out, w_in, acc_in, acc_out, acc_bi, acc_bo):
    half, square = gelu_half(pre)
    act = pre * half
    slope = half + act * (1.0 - half) * (2.0 * C0 + (6.0 * C0 * C1) * square)
    act = act.astype(BF16)
    delta = (dot(w_out[...], back) * slope).astype(BF16)
    grad = back.astype(F32) + dot(w_in, delta)
    ones = jnp.ones((TRACK_W, BLOCK), BF16)
    acc_in[...] += dot(u, delta, NT)
    acc_out[...] += dot(back, act, NT)
    acc_bi[...] += dot(ones, delta, NT)
    acc_bo[...] += dot(ones, back, NT)
    return act, grad


def put_sums(out, scale, acc_in, acc_out, acc_bi, acc_bo, bias):
    width, hidden = acc_in.shape
    for which, acc in enumerate((acc_in, acc_out)):
        for j in range(hidden // LANES):
            lo = (which * (hidden // LANES) + j) * width
            out[lo : lo + width, :] = (acc[:, j * LANES : (j + 1) * LANES] * scale).astype(BF16)
    lo = 2 * (hidden // LANES) * width
    out[lo:, :] = jnp.zeros((out.shape[0] - lo, LANES), BF16)
    bias[...] = jnp.zeros_like(bias)
    at = 0
    for acc in (acc_bi, acc_bo):
        n = acc.shape[1]
        for j in range(0, n, LANES):
            size = min(LANES, n - j)
            bias[at : at + 1, 0:size] = acc[0:1, j : j + size] * scale
            at += 1
    out[lo : lo + TRACK_W, :] = bias[...].astype(BF16)


def zero(*refs):
    for ref in refs:
        ref[...] = jnp.zeros_like(ref)


def middle_kernel(scale, *refs):
    un, uf, cot, bf, shared = *refs[0:4], refs[16]
    ufar, bfar = sorted_far(refs[4:16:2]), sorted_far(refs[5:16:2])
    w_in, b_in, w_out_t, b_out = refs[17:21]
    mn, mf, mfar, gn, gf, gfar, passing, sums = refs[21], refs[22], refs[23:29], refs[29], refs[30], refs[31:37], refs[37], refs[38]
    u_all, back_all, w_in_t, w_out, wide_in, wide_out, acc_in, acc_out, acc_bi, acc_bo, bias = refs[39:]
    w_in_t[...] = turned(w_in[1])
    w_out[...] = turned(w_out_t[1])
    wide_in[...] = column(b_in[1:2, :])
    wide_out[...] = column(b_out[1:2, :])
    assemble(u_all, un, uf, (*ufar, shared.at[0:TRACK_W]), 1)
    assemble(back_all, cot, bf, (*bfar, shared.at[TRACK_W : 2 * TRACK_W]), -1)
    zero(acc_in, acc_out, acc_bi, acc_bo)

    def body(at):
        u, back = u_all[:, at], back_all[:, at]
        pre = dot(w_in_t[...], u) + across(wide_in[...])
        act, grad = backward(u, back, pre, w_out, w_in[1], acc_in, acc_out, acc_bi, acc_bo)
        put_pieces(grad.astype(BF16), at, gn, gf, (*gfar, passing.at[TRACK_W : 2 * TRACK_W]))
        mixed = u.astype(F32) + dot(w_out_t[1], act) + across(wide_out[...])
        put_pieces(mixed.astype(BF16), at, mn, mf, (*mfar, passing.at[0:TRACK_W]))

    over_blocks(un.shape[1], body)
    put_margins(gn, gf, -1)
    put_margins(mn, mf, 1)
    put_sums(sums, scale, acc_in, acc_out, acc_bi, acc_bo, bias)


def last_kernel(scale, tokens, w_in, b_in, w_out_t, sums1, *refs):
    bn, bf, bfar, shared = refs[0], refs[1], sorted_far(refs[2:8]), refs[8]
    grad_tokens, keep, send, w_in_t, w_out, back_all, wide_in, acc_in, acc_out, acc_bi, acc_bo, bias = refs[9:]
    core = lax.axis_index("c")
    zero(acc_in, acc_out, acc_bi, acc_bo)
    w_in_t[...] = turned(w_in[0])
    w_out[...] = turned(w_out_t[0])
    wide_in[...] = column(b_in[0:1, :])
    assemble(back_all, bn, bf, (*bfar, shared.at[TRACK_W : 2 * TRACK_W]), -1)

    def body(at):
        u, back = tokens[:, at], back_all[:, at]
        pre = dot(w_in_t[...], u) + across(wide_in[...])
        _, grad = backward(u, back, pre, w_out, w_in[0], acc_in, acc_out, acc_bi, acc_bo)
        grad_tokens[:, at] = grad.astype(BF16)

    over_blocks(tokens.shape[1], body)

    @pl.when(core == 0)
    def _():
        put_sums(keep, scale, acc_in, acc_out, acc_bi, acc_bo, bias)
        send[...] = sums1[...]

    @pl.when(core != 0)
    def _():
        put_sums(send, scale, acc_in, acc_out, acc_bi, acc_bo, bias)
        keep[...] = sums1[...]


def join_kernel(near, first, *refs):
    assemble(refs[7], near, first, (*sorted_far(refs[:6]), refs[6].at[0:TRACK_W]), 1)


def sum_kernel(parts, out):
    total = parts[0].astype(F32)
    for i in range(1, parts.shape[0]):
        total += parts[i].astype(F32)
    for j in range(out.shape[0]):
        out[j] = total.astype(BF16)


def spread_kernel(width, hidden, mine, other, w_in, b_in, w_out_t, b_out, bias):
    blocks = hidden // LANES

    def layer_from(layer, ref):
        for j in range(blocks):
            columns = slice(j * LANES, (j + 1) * LANES)
            w_in[layer, :, columns] = ref[j * width : (j + 1) * width, :].astype(F32)
            lo = (blocks + j) * width
            w_out_t[layer, :, columns] = ref[lo : lo + width, :].astype(F32)
        lo = 2 * blocks * width
        bias[...] = ref[lo : lo + TRACK_W, :].astype(F32)
        at = 0
        for out, n in ((b_in, hidden), (b_out, width)):
            for j in range(0, n, LANES):
                size = min(LANES, n - j)
                out[layer : layer + 1, j : j + size] = bias[at : at + 1, 0:size]
                at += 1

    @pl.when(lax.axis_index("c") == 0)
    def _():
        layer_from(0, mine)
        layer_from(1, other)

    @pl.when(lax.axis_index("c") != 0)
    def _():
        layer_from(0, other)
        layer_from(1, mine)


def call(kernel, outs, args, scratch=(), flops=0, moved=0, hbm=0, mib=24):
    vmem = pl.BlockSpec(memory_space=pltpu.VMEM)
    return pl.pallas_call(
        kernel,
        out_shape=outs,
        in_specs=[pl.BlockSpec(memory_space=pltpu.HBM)] * hbm + [vmem] * (len(args) - hbm),
        out_specs=jax.tree.map(lambda _: vmem, outs),
        scratch_shapes=list(scratch),
        cost_estimate=pl.CostEstimate(flops=flops, bytes_accessed=moved, transcendentals=0),
        compiler_params=pltpu.CompilerParams(vmem_limit_bytes=mib * 1024 * 1024),
    )(*args)


def passed(block, distance):
    n = lax.axis_size(ALL)
    return lax.ppermute(block, ALL, [((i - distance) % n, i) for i in range(n)])


def transfer(first, far, sign):
    return passed(first, sign), [passed(far[i], sign * HOPS[i + 1]) for i in ORDER]


def sorted_far(far):
    return [far[ORDER.index(i)] for i in range(len(ORDER))]


def local(tokens, w_in, b_in, w_out, b_out, cotangent):
    rows, width = tokens.shape
    layers, _, hidden = w_in.shape
    devices = range(lax.axis_size(ALL))
    scale = 1.0 / (rows * len(devices)) ** 0.5
    shape = jax.ShapeDtypeStruct
    near = shape((NEAR * TRACK_W, rows), BF16)
    first = shape((TRACK_W, margins(rows)[1]), BF16)
    far = [shape((TRACK_W, rows), BF16)] * (len(HOPS) - 2)
    shared = shape((2 * TRACK_W, rows), BF16)
    sums = shape((3328, LANES), BF16)
    whole = pltpu.VMEM((width, rows), BF16)
    weight = pltpu.VMEM((hidden, width), BF16)
    wide_in, wide_out = pltpu.VMEM((hidden, LANES), F32), pltpu.VMEM((width, LANES), F32)
    accs = [
        pltpu.VMEM((width, hidden), F32),
        pltpu.VMEM((width, hidden), F32),
        pltpu.VMEM((TRACK_W, hidden), F32),
        pltpu.VMEM((TRACK_W, width), F32),
        pltpu.VMEM((TRACK_W, LANES), F32),
    ]
    product = 2 * rows * width * hidden
    block = 2 * rows * width
    tokens, cotangent = tokens.T, cotangent.T
    w_out_t = jnp.swapaxes(w_out, 1, 2)
    outs = call(
        first_kernel,
        [near, first, *far, first, *far, shared],
        (tokens, cotangent, w_in, b_in, w_out_t, b_out),
        [
            whole,
            pltpu.VMEM((width, hidden), BF16),
            weight,
            pltpu.VMEM((width, hidden), BF16),
            pltpu.VMEM((layers, hidden), F32),
            pltpu.VMEM((layers, width), F32),
            wide_in,
            wide_out,
            pltpu.SemaphoreType.DMA((6 + len(HOPS) - 1 + NEAR - 1,)),
        ],
        flops=4 * product,
        moved=4 * block,
        hbm=6,
        mib=60,
    )
    shared0 = passed(outs[15], HOPS[-1])
    near_u, (first_u, far_u) = outs[0], transfer(outs[1], outs[2:8], 1)
    first_b, far_b = transfer(outs[8], outs[9:15], -1)
    both = [v for pair in zip(far_u, far_b) for v in pair]
    outs = call(
        functools.partial(middle_kernel, scale),
        [near, first, *far, near, first, *far, shared, sums],
        (near_u, first_u, cotangent, first_b, *both, shared0, w_in, b_in, w_out_t, b_out),
        [whole, whole, weight, weight, wide_in, wide_out] + accs,
        flops=12 * product,
        moved=4 * block,
    )
    shared1, sums1 = passed(outs[16], HOPS[-1]), outs[17]
    first_b, far_b = transfer(outs[9], outs[10:16], -1)
    back0 = (outs[8], first_b, *far_b)
    first_u, far_u = transfer(outs[1], outs[2:8], 1)
    shifted = (outs[0], first_u, *far_u)
    grad_tokens, keep, send = call(
        functools.partial(last_kernel, scale),
        [shape((width, rows), BF16), sums, sums],
        (tokens, w_in, b_in, w_out_t, sums1, *back0, shared1),
        [weight, weight, whole, wide_in, *accs],
        flops=10 * product,
        moved=3 * block,
    )
    send, *shifted = lax.optimization_barrier((send, *shifted))
    partner = lax.ppermute(send, ALL, [(i ^ 1, i) for i in devices])
    result = call(join_kernel, shape((width, rows), BF16), (*shifted, shared1), flops=product // 4, moved=2 * block)
    plane = lax.axis_size(("x", "y"))
    depth = lax.axis_size("z")
    part = (keep.astype(F32) + partner.astype(F32)).astype(BF16).reshape(plane, -1, LANES)
    part = lax.all_to_all(part, ("x", "y"), 0, 0, tiled=True)
    part = call(sum_kernel, shape((depth, *part.shape[1:]), BF16), (part,), flops=block, moved=block, mib=8)
    part = lax.all_to_all(part, "z", 0, 0, tiled=True)
    part = call(sum_kernel, shape((plane, *part.shape[1:]), BF16), (part,), flops=block, moved=block, mib=8)
    mine = lax.all_to_all(part, ("x", "y"), 0, 0, tiled=True).reshape(-1, LANES)
    other = lax.ppermute(mine, ALL, [(i ^ 1, i) for i in devices])
    gw_in, gb_in, gw_out_t, gb_out = call(
        functools.partial(spread_kernel, width, hidden),
        [
            shape((layers, width, hidden), F32),
            shape((layers, hidden), F32),
            shape((layers, width, hidden), F32),
            shape((layers, width), F32),
        ],
        (mine, other),
        [pltpu.VMEM((TRACK_W, LANES), F32)],
        flops=product // 4,
        moved=4 * block,
    )
    return result.T, grad_tokens.T, gw_in, gb_in, jnp.swapaxes(gw_out_t, 1, 2), gb_out


def solution(mesh):
    split = Mesh(mesh.devices.reshape(4, 4, 8, 2), ALL)
    rows = P(ALL, None)
    return jax.shard_map(
        local,
        mesh=split,
        in_specs=(rows, P(), P(), P(), P(), rows),
        out_specs=(rows, rows, P(), P(), P(), P()),
        check_vma=False,
    )
```

```python
import functools

import jax
import jax.numpy as jnp
from jax import lax
from jax.experimental import pallas as pl
from jax.experimental.pallas import tpu as pltpu
from jax.sharding import Mesh
from jax.sharding import PartitionSpec as P

TRACK_W = 16
TRACKS = 20
NEAR = 12
HOPS = (1, 2, 4, 8, 16, 32, 64, 128)
ALL = ("x", "y", "z", "c")
BLOCK = 512
LANES = 128
C0 = 0.7978845608028654
C1 = 0.044715
BF16 = jnp.bfloat16
F32 = jnp.float32

NT = (((1,), (1,)), ((), ()))
NN = (((1,), (0,)), ((), ()))


def dot(a, b, dims=NN):
    return lax.dot_general(a, b, dims, preferred_element_type=F32)


def margins(rows):
    out, at = [], rows
    for track in range(1, NEAR):
        size = max(LANES, 2 ** (track - 1))
        out.append((track, size, at))
        at += size
    return out, at


def put_pieces(v, at, near, first, far):
    near[:, at] = v[: NEAR * TRACK_W]
    put_far(v, at, first, far)


def put_far(v, at, first, far):
    top = NEAR * TRACK_W
    first[:, at] = v[top : top + TRACK_W]
    for i, ref in enumerate(far):
        lo = top + TRACK_W * (i + 1)
        ref[:, at] = v[lo : lo + TRACK_W]


def put_margins(near, first, sign):
    rows = near.shape[1]
    for track, size, at in margins(rows)[0]:
        lo = rows - size if sign > 0 else 0
        first[:, at : at + size] = near[track * TRACK_W : (track + 1) * TRACK_W, lo : lo + size]


def assemble(out, near, first, far, sign):
    rows = near.shape[1]
    out[0:TRACK_W, :] = near[0:TRACK_W, :]
    lane = lax.broadcasted_iota(jnp.int32, (TRACK_W, LANES), 1)
    for track, size, at in margins(rows)[0]:
        shift = 2 ** (track - 1)
        own = slice(track * TRACK_W, (track + 1) * TRACK_W)
        if shift < LANES:
            values = near[own, :].astype(F32)
            edge = first[:, at : at + LANES].astype(F32)
            if sign > 0:
                moved = pltpu.roll(values, shift, 1)
                edge = pltpu.roll(edge, shift, 1)
                head = jnp.where(lane < shift, edge, moved[:, :LANES])
                out[own, 0:LANES] = head.astype(BF16)
                out[own, LANES:rows] = moved[:, LANES:].astype(BF16)
            else:
                moved = pltpu.roll(values, rows - shift, 1)
                edge = pltpu.roll(edge, LANES - shift, 1)
                tail = jnp.where(lane >= LANES - shift, edge, moved[:, rows - LANES :])
                out[own, 0 : rows - LANES] = moved[:, : rows - LANES].astype(BF16)
                out[own, rows - LANES : rows] = tail.astype(BF16)
        elif sign > 0:
            out[own, 0:shift] = first[:, at : at + shift]
            out[own, shift:rows] = near[own, 0 : rows - shift]
        else:
            out[own, 0 : rows - shift] = near[own, shift:rows]
            out[own, rows - shift : rows] = first[:, at : at + shift]
    top = NEAR * TRACK_W
    out[top : top + TRACK_W, :] = first[:, 0:rows]
    for i, ref in enumerate(far):
        lo = top + TRACK_W * (i + 1)
        out[lo : lo + TRACK_W, :] = ref[...]


def over_blocks(rows, body):
    def step(i, carry):
        body(pl.ds(pl.multiple_of(i * BLOCK, BLOCK), BLOCK))
        return carry

    lax.fori_loop(0, rows // BLOCK, step, 0)


def column(row):
    wide = jnp.broadcast_to(row, (LANES, row.shape[1])).T
    return wide


def across(wide):
    return jnp.concatenate([wide] * (BLOCK // LANES), axis=1)


def turned(x):
    return x.astype(F32).T.astype(BF16)


def gelu_half(t):
    square = t * t
    return 0.5 + 0.5 * jnp.tanh(t * (C0 + (C0 * C1) * square)), square


def brought(sems, pairs):
    copies = [pltpu.make_async_copy(source, target, sems.at[i]) for i, (source, target) in enumerate(pairs)]
    for copy in copies:
        copy.start()
    return copies


def first_kernel(tokens, cot, w_in, b_in, w_out_t, b_out, *refs):
    near, first, far, cot_first, cot_far, shared = refs[0], refs[1], refs[2:8], refs[8], refs[9:15], refs[15]
    x_all, w_here, w_in_t, w_out_here, b_in_here, b_out_here, wide_in, wide_out, sems = refs[16:]
    rows = tokens.shape[1]
    up, down = shared.at[0:TRACK_W], shared.at[TRACK_W : 2 * TRACK_W]
    top = NEAR * TRACK_W
    pairs = [
        (w_in.at[0], w_here),
        (b_in, b_in_here),
        (tokens, x_all),
        (w_out_t.at[0], w_out_here),
        (b_out, b_out_here),
        (cot.at[top : top + TRACK_W], cot_first.at[:, 0:rows]),
    ]
    for i, ref in enumerate((*cot_far, down)):
        lo = top + TRACK_W * (i + 1)
        pairs.append((cot.at[lo : lo + TRACK_W], ref))
    for track, size, at in margins(rows)[0]:
        own = slice(track * TRACK_W, (track + 1) * TRACK_W)
        pairs.append((cot.at[own, 0:size], cot_first.at[:, at : at + size]))
    copies = brought(sems, pairs)
    copies[0].wait()
    w_in_t[...] = turned(w_here[...])
    copies[1].wait()
    wide_in[...] = column(b_in_here[0:1, :])
    for copy in copies[2:5]:
        copy.wait()
    wide_out[...] = column(b_out_here[0:1, :])

    def body(at):
        x = x_all[:, at]
        pre = dot(w_in_t[...], x) + across(wide_in[...])
        act = (pre * gelu_half(pre)[0]).astype(BF16)
        mixed = x.astype(F32) + dot(w_out_here[...], act) + across(wide_out[...])
        put_pieces(mixed.astype(BF16), at, near, first, (*far, up))

    over_blocks(rows, body)
    put_margins(near, first, 1)
    for copy in copies[5:]:
        copy.wait()


def backward(u, back, pre, w_out, w_in, acc_in, acc_out, acc_bi, acc_bo):
    half, square = gelu_half(pre)
    act = pre * half
    slope = half + act * (1.0 - half) * (2.0 * C0 + (6.0 * C0 * C1) * square)
    act = act.astype(BF16)
    delta = (dot(w_out[...], back) * slope).astype(BF16)
    grad = back.astype(F32) + dot(w_in, delta)
    ones = jnp.ones((TRACK_W, BLOCK), BF16)
    acc_in[...] += dot(u, delta, NT)
    acc_out[...] += dot(back, act, NT)
    acc_bi[...] += dot(ones, delta, NT)
    acc_bo[...] += dot(ones, back, NT)
    return act, grad


def put_sums(out, scale, acc_in, acc_out, acc_bi, acc_bo, bias):
    width, hidden = acc_in.shape
    for which, acc in enumerate((acc_in, acc_out)):
        for j in range(hidden // LANES):
            lo = (which * (hidden // LANES) + j) * width
            out[lo : lo + width, :] = (acc[:, j * LANES : (j + 1) * LANES] * scale).astype(BF16)
    lo = 2 * (hidden // LANES) * width
    out[lo:, :] = jnp.zeros((out.shape[0] - lo, LANES), BF16)
    bias[...] = jnp.zeros_like(bias)
    at = 0
    for acc in (acc_bi, acc_bo):
        n = acc.shape[1]
        for j in range(0, n, LANES):
            size = min(LANES, n - j)
            bias[at : at + 1, 0:size] = acc[0:1, j : j + size] * scale
            at += 1
    out[lo : lo + TRACK_W, :] = bias[...].astype(BF16)


def zero(*refs):
    for ref in refs:
        ref[...] = jnp.zeros_like(ref)


def middle_kernel(scale, *refs):
    un, uf, ufar, cot, bf, bfar, shared = refs[0], refs[1], refs[2:8], refs[8], refs[9], refs[10:16], refs[16]
    w_in, b_in, w_out_t, b_out = refs[17:21]
    mn, mf, mfar, gn, gf, gfar, passing, sums = refs[21], refs[22], refs[23:29], refs[29], refs[30], refs[31:37], refs[37], refs[38]
    u_all, back_all, w_in_t, w_out, wide_in, wide_out, acc_in, acc_out, acc_bi, acc_bo, bias = refs[39:]
    w_in_t[...] = turned(w_in[1])
    w_out[...] = turned(w_out_t[1])
    wide_in[...] = column(b_in[1:2, :])
    wide_out[...] = column(b_out[1:2, :])
    assemble(u_all, un, uf, (*ufar, shared.at[0:TRACK_W]), 1)
    assemble(back_all, cot, bf, (*bfar, shared.at[TRACK_W : 2 * TRACK_W]), -1)
    zero(acc_in, acc_out, acc_bi, acc_bo)

    def body(at):
        u, back = u_all[:, at], back_all[:, at]
        pre = dot(w_in_t[...], u) + across(wide_in[...])
        act, grad = backward(u, back, pre, w_out, w_in[1], acc_in, acc_out, acc_bi, acc_bo)
        put_pieces(grad.astype(BF16), at, gn, gf, (*gfar, passing.at[TRACK_W : 2 * TRACK_W]))
        mixed = u.astype(F32) + dot(w_out_t[1], act) + across(wide_out[...])
        put_pieces(mixed.astype(BF16), at, mn, mf, (*mfar, passing.at[0:TRACK_W]))

    over_blocks(un.shape[1], body)
    put_margins(gn, gf, -1)
    put_margins(mn, mf, 1)
    put_sums(sums, scale, acc_in, acc_out, acc_bi, acc_bo, bias)


def last_kernel(scale, tokens, w_in, b_in, w_out_t, sums1, *refs):
    bn, bf, bfar, shared = refs[0], refs[1], refs[2:8], refs[8]
    grad_tokens, keep, send, w_in_t, w_out, back_all, wide_in, acc_in, acc_out, acc_bi, acc_bo, bias = refs[9:]
    core = lax.axis_index("c")
    zero(acc_in, acc_out, acc_bi, acc_bo)
    w_in_t[...] = turned(w_in[0])
    w_out[...] = turned(w_out_t[0])
    wide_in[...] = column(b_in[0:1, :])
    assemble(back_all, bn, bf, (*bfar, shared.at[TRACK_W : 2 * TRACK_W]), -1)

    def body(at):
        u, back = tokens[:, at], back_all[:, at]
        pre = dot(w_in_t[...], u) + across(wide_in[...])
        _, grad = backward(u, back, pre, w_out, w_in[0], acc_in, acc_out, acc_bi, acc_bo)
        grad_tokens[:, at] = grad.astype(BF16)

    over_blocks(tokens.shape[1], body)

    @pl.when(core == 0)
    def _():
        put_sums(keep, scale, acc_in, acc_out, acc_bi, acc_bo, bias)
        send[...] = sums1[...]

    @pl.when(core != 0)
    def _():
        put_sums(send, scale, acc_in, acc_out, acc_bi, acc_bo, bias)
        keep[...] = sums1[...]


def join_kernel(near, first, *refs):
    assemble(refs[7], near, first, (*refs[:6], refs[6].at[0:TRACK_W]), 1)


def sum_kernel(parts, out):
    total = parts[0].astype(F32)
    for i in range(1, parts.shape[0]):
        total += parts[i].astype(F32)
    for j in range(out.shape[0]):
        out[j] = total.astype(BF16)


def spread_kernel(width, hidden, mine, other, w_in, b_in, w_out_t, b_out, bias):
    blocks = hidden // LANES

    def layer_from(layer, ref):
        for j in range(blocks):
            columns = slice(j * LANES, (j + 1) * LANES)
            w_in[layer, :, columns] = ref[j * width : (j + 1) * width, :].astype(F32)
            lo = (blocks + j) * width
            w_out_t[layer, :, columns] = ref[lo : lo + width, :].astype(F32)
        lo = 2 * blocks * width
        bias[...] = ref[lo : lo + TRACK_W, :].astype(F32)
        at = 0
        for out, n in ((b_in, hidden), (b_out, width)):
            for j in range(0, n, LANES):
                size = min(LANES, n - j)
                out[layer : layer + 1, j : j + size] = bias[at : at + 1, 0:size]
                at += 1

    @pl.when(lax.axis_index("c") == 0)
    def _():
        layer_from(0, mine)
        layer_from(1, other)

    @pl.when(lax.axis_index("c") != 0)
    def _():
        layer_from(0, other)
        layer_from(1, mine)


def call(kernel, outs, args, scratch=(), flops=0, moved=0, hbm=0, mib=24):
    vmem = pl.BlockSpec(memory_space=pltpu.VMEM)
    return pl.pallas_call(
        kernel,
        out_shape=outs,
        in_specs=[pl.BlockSpec(memory_space=pltpu.HBM)] * hbm + [vmem] * (len(args) - hbm),
        out_specs=jax.tree.map(lambda _: vmem, outs),
        scratch_shapes=list(scratch),
        cost_estimate=pl.CostEstimate(flops=flops, bytes_accessed=moved, transcendentals=0),
        compiler_params=pltpu.CompilerParams(vmem_limit_bytes=mib * 1024 * 1024),
    )(*args)


def passed(block, distance):
    n = lax.axis_size(ALL)
    return lax.ppermute(block, ALL, [((i - distance) % n, i) for i in range(n)])


def transfer(first, far, sign):
    far = [passed(v, sign * hop) for v, hop in zip(far, HOPS[1:-1])]
    return (passed(first, sign), *far)


def local(tokens, w_in, b_in, w_out, b_out, cotangent):
    rows, width = tokens.shape
    layers, _, hidden = w_in.shape
    devices = range(lax.axis_size(ALL))
    scale = 1.0 / (rows * len(devices)) ** 0.5
    shape = jax.ShapeDtypeStruct
    near = shape((NEAR * TRACK_W, rows), BF16)
    first = shape((TRACK_W, margins(rows)[1]), BF16)
    far = [shape((TRACK_W, rows), BF16)] * (len(HOPS) - 2)
    shared = shape((2 * TRACK_W, rows), BF16)
    sums = shape((3328, LANES), BF16)
    whole = pltpu.VMEM((width, rows), BF16)
    weight = pltpu.VMEM((hidden, width), BF16)
    wide_in, wide_out = pltpu.VMEM((hidden, LANES), F32), pltpu.VMEM((width, LANES), F32)
    accs = [
        pltpu.VMEM((width, hidden), F32),
        pltpu.VMEM((width, hidden), F32),
        pltpu.VMEM((TRACK_W, hidden), F32),
        pltpu.VMEM((TRACK_W, width), F32),
        pltpu.VMEM((TRACK_W, LANES), F32),
    ]
    product = 2 * rows * width * hidden
    block = 2 * rows * width
    tokens, cotangent = tokens.T, cotangent.T
    w_out_t = jnp.swapaxes(w_out, 1, 2)
    outs = call(
        first_kernel,
        [near, first, *far, first, *far, shared],
        (tokens, cotangent, w_in, b_in, w_out_t, b_out),
        [
            whole,
            pltpu.VMEM((width, hidden), BF16),
            weight,
            pltpu.VMEM((width, hidden), BF16),
            pltpu.VMEM((layers, hidden), F32),
            pltpu.VMEM((layers, width), F32),
            wide_in,
            wide_out,
            pltpu.SemaphoreType.DMA((6 + len(HOPS) - 1 + NEAR - 1,)),
        ],
        flops=4 * product,
        moved=4 * block,
        hbm=6,
        mib=60,
    )
    shared0 = passed(outs[15], HOPS[-1])
    u1 = (outs[0], *transfer(outs[1], outs[2:8], 1))
    back1 = (cotangent, *transfer(outs[8], outs[9:15], -1))
    outs = call(
        functools.partial(middle_kernel, scale),
        [near, first, *far, near, first, *far, shared, sums],
        (*u1, *back1, shared0, w_in, b_in, w_out_t, b_out),
        [whole, whole, weight, weight, wide_in, wide_out] + accs,
        flops=12 * product,
        moved=4 * block,
    )
    shared1, sums1 = passed(outs[16], HOPS[-1]), outs[17]
    back0 = (outs[8], *transfer(outs[9], outs[10:16], -1))
    shifted = (outs[0], *transfer(outs[1], outs[2:8], 1))
    grad_tokens, keep, send = call(
        functools.partial(last_kernel, scale),
        [shape((width, rows), BF16), sums, sums],
        (tokens, w_in, b_in, w_out_t, sums1, *back0, shared1),
        [weight, weight, whole, wide_in, *accs],
        flops=10 * product,
        moved=3 * block,
    )
    send, *shifted = lax.optimization_barrier((send, *shifted))
    partner = lax.ppermute(send, ALL, [(i ^ 1, i) for i in devices])
    result = call(join_kernel, shape((width, rows), BF16), (*shifted, shared1), flops=product // 4, moved=2 * block)
    plane = lax.axis_size(("x", "y"))
    depth = lax.axis_size("z")
    part = (keep.astype(F32) + partner.astype(F32)).astype(BF16).reshape(plane, -1, LANES)
    part = lax.all_to_all(part, ("x", "y"), 0, 0, tiled=True)
    part = call(sum_kernel, shape((depth, *part.shape[1:]), BF16), (part,), flops=block, moved=block, mib=8)
    part = lax.all_to_all(part, "z", 0, 0, tiled=True)
    part = call(sum_kernel, shape((plane, *part.shape[1:]), BF16), (part,), flops=block, moved=block, mib=8)
    mine = lax.all_to_all(part, ("x", "y"), 0, 0, tiled=True).reshape(-1, LANES)
    other = lax.ppermute(mine, ALL, [(i ^ 1, i) for i in devices])
    gw_in, gb_in, gw_out_t, gb_out = call(
        functools.partial(spread_kernel, width, hidden),
        [
            shape((layers, width, hidden), F32),
            shape((layers, hidden), F32),
            shape((layers, width, hidden), F32),
            shape((layers, width), F32),
        ],
        (mine, other),
        [pltpu.VMEM((TRACK_W, LANES), F32)],
        flops=product // 4,
        moved=4 * block,
    )
    return result.T, grad_tokens.T, gw_in, gb_in, jnp.swapaxes(gw_out_t, 1, 2), gb_out


def solution(mesh):
    split = Mesh(mesh.devices.reshape(4, 4, 8, 2), ALL)
    rows = P(ALL, None)
    return jax.shard_map(
        local,
        mesh=split,
        in_specs=(rows, P(), P(), P(), P(), rows),
        out_specs=(rows, rows, P(), P(), P(), P()),
        check_vma=False,
    )
```
